32 devices in a mesh: rep: 2 (over y), seq: 4 (over z), tp: 4 (over x, core).
Axes of the slice: x: 2, y: 2, z: 4, core: 2. Of those that a mesh axis runs over, the one named last changes fastest.
Arguments:
- queries: bfloat16 [128, 64, 128], P(('rep', 'seq')), parts along dimension 0, may hold values from -9 to 9
- key_pages: bfloat16 [1024, 8, 64, 128], P(('rep', 'seq'), 'tp'), parts along dimension 0, may hold values from -4 to 4
- value_pages: bfloat16 [1024, 8, 64, 128], P(('rep', 'seq'), 'tp'), parts along dimension 0, may hold values from -6 to 6
- page_owner: int32 [128, 128], P('rep'), parts along dimension 0, may hold values from 0 to 3, as said below
- page_local: int32 [128, 128], P('rep'), parts along dimension 0, may hold values from 0 to 127, as said below
- seq_lengths: int32 [128], P('rep'), parts along dimension 0, may hold values from 1 to 8192, as said below
Outputs:
- attention: bfloat16 [128, 64, 128], P(('rep', 'seq'), 'tp'), parts along dimension 0
The draws below stay inside these ranges and needn't reach their ends.
There are 2 independent parts, one for each index of `rep`. The reference program is written for one: setup_inputs(seed, part) draws one part's arguments, and reference() takes and returns one part's arrays. A program takes and returns all parts, laid end to end along the dimension named above; each array names one. Nothing has to cross between parts.
Inputs may be any that keep to these rules, and one draw needn't show every extreme that they name: The live slots (s * 64 < seq_lengths[b]) name pairs (page_owner, page_local) that are all different; the other slots hold 0. `page_local`: see page_owner. `seq_lengths`: one sequence has exactly 8192 tokens; the live slots of all sequences together number at most half of the 512 pages.
All inputs are finite; a program needn't handle non-finite values.
Results may differ from the reference program's by a relative error of at most 0.008.
Values may be sent and summed in bfloat16 or wider, within the bound.
No kernel may reach another device: no remote copies, remote signals or barrier semaphores. Data moves between devices by JAX's collectives and lax.ppermute only.
A program may use at most 64 MiB of HBM per device.

```python
import math
import jax
import jax.numpy as jnp
from jax import lax

HQ = 64
KVH = 8
HD = 128
PAGE = 64
SEQS = 64
P_DEV = 128
POOL = 512
MAXP = 128
N_SEQ = 4


def page_layout(key):
    base = jax.random.fold_in(key, 7)
    keys_list = jax.random.split(base, 5)
    longest = jax.random.randint(keys_list[0], (), 0, SEQS)
    upper = max(1, POOL // (4 * (SEQS - 1)))
    seq_index = jnp.arange(SEQS, dtype=jnp.int32)
    page_count = jax.random.randint(keys_list[1], (SEQS,), 1, upper + 1)
    page_count = jnp.where(seq_index == longest, MAXP, page_count).astype(jnp.int32)
    last_fill = jax.random.randint(keys_list[2], (SEQS,), 1, PAGE + 1)
    last_fill = jnp.where(seq_index == longest, PAGE, last_fill).astype(jnp.int32)
    lengths = (page_count - 1) * PAGE + last_fill
    slot_ids = jnp.arange(MAXP, dtype=jnp.int32)
    used = (slot_ids[None, :] < page_count[:, None]).reshape(-1).astype(jnp.int32)
    ordinal = jnp.cumsum(used) - 1
    device_weight = jax.random.randint(keys_list[3], (N_SEQ,), 1, 17)
    raw_score = jax.random.randint(keys_list[4], (POOL,), 0, 65536)
    pool_ids = jnp.arange(POOL, dtype=jnp.int32)
    score = raw_score // device_weight[pool_ids // P_DEV] * POOL + pool_ids
    pool_order = jnp.argsort(score).astype(jnp.int32)
    target = pool_order[jnp.clip(ordinal, 0, POOL - 1)]
    target = jnp.where(used > 0, target, 0).reshape(SEQS, MAXP)
    return (lengths.astype(jnp.int32), (target // P_DEV).astype(jnp.int32), (target % P_DEV).astype(jnp.int32))


def draw_seq_lengths(key, part):
    return page_layout(key)[0]


def draw_page_owner(key, part):
    return page_layout(key)[1]


def draw_page_local(key, part):
    return page_layout(key)[2]


def draw_queries(key, part):
    values = jax.random.truncated_normal(key, -4.0, 4.0, (SEQS, HQ, HD), jnp.float32)
    row_scale = jnp.exp(jax.random.uniform(jax.random.fold_in(key, 3), (SEQS, 1, 1), jnp.float32, -0.7, 0.7))
    return (values * row_scale).astype(jnp.bfloat16)


def block_levels(key, dims, cuts, smallest, top_value):
    gain = 1.0
    for axis_at, parts in cuts:
        draws = jax.random.uniform(jax.random.fold_in(jax.random.fold_in(key, 6), axis_at), (parts,), jnp.float32, smallest / len(cuts), top_value / len(cuts))
        gain = gain * jnp.repeat(jnp.exp(draws), dims[axis_at] // parts).reshape((-1,) + (1,) * (len(dims) - 1 - axis_at))
    return gain


def bell_draw(rng, extent, scale, most, cuts=(), kind=jnp.bfloat16):
    loudness = block_levels(rng, extent, cuts, -0.22, 0.18) if cuts else 1.0
    values = jax.random.normal(rng, extent, jnp.float32) * scale * loudness
    return jnp.minimum(jnp.maximum(values, -most), most).astype(kind)


def setup_inputs(seed: int = 0, part: int = 0) -> dict:
    arg_keys = jax.random.split(jax.random.key(seed), 7)
    own_keys = jax.random.split(jax.random.fold_in(arg_keys[6], part), 7)
    queries = draw_queries(jax.random.fold_in(jax.random.fold_in(arg_keys[6], part), 71), part)
    key_pages = bell_draw(own_keys[1], (POOL, KVH, PAGE, HD), 1.0, 4.0, ((0, 4), (1, 4)))
    value_pages = bell_draw(own_keys[2], (POOL, KVH, PAGE, HD), 1.0, 6.0, ((0, 4), (1, 4)))
    page_owner = draw_page_owner(jax.random.fold_in(jax.random.fold_in(arg_keys[6], part), 71), part)
    page_local = draw_page_local(jax.random.fold_in(jax.random.fold_in(arg_keys[6], part), 71), part)
    seq_lengths = draw_seq_lengths(jax.random.fold_in(jax.random.fold_in(arg_keys[6], part), 71), part)
    return dict(queries=queries, key_pages=key_pages, value_pages=value_pages, page_owner=page_owner, page_local=page_local, seq_lengths=seq_lengths)


score_shift = 8.0

def reference(queries, key_pages, value_pages, page_owner, page_local, seq_lengths):
    group_size = HQ // KVH
    slot_ids = jnp.arange(MAXP, dtype=jnp.int32)
    slot_fill = jnp.clip(seq_lengths[:, None] - slot_ids[None, :] * PAGE, 0, PAGE).astype(jnp.int32)
    pool_index = (page_owner * P_DEV + page_local).astype(jnp.int32)
    target = jnp.where(slot_fill > 0, pool_index, POOL).astype(jnp.int32).reshape(-1)
    seq_ids = jnp.broadcast_to(jnp.arange(SEQS, dtype=jnp.int32)[:, None], (SEQS, MAXP)).reshape(-1)
    page_seq = jnp.zeros((POOL,), jnp.int32).at[target].set(seq_ids, mode='drop')
    page_fill = jnp.zeros((POOL,), jnp.int32).at[target].set(slot_fill.reshape(-1), mode='drop')
    block_pages = math.gcd(POOL, 64)
    block_count = POOL // block_pages
    key_blocks = key_pages.reshape(block_count, block_pages, KVH, PAGE, HD)
    value_blocks = value_pages.reshape(block_count, block_pages, KVH, PAGE, HD)
    seq_blocks = page_seq.reshape(block_count, block_pages)
    fill_blocks = page_fill.reshape(block_count, block_pages)
    score_scale = 1.0 / math.sqrt(HD)

    def visit(carry, block):
        numerator, denominator = carry
        key_block, value_block, seq_block, fill_block = block
        picked = queries[seq_block].astype(jnp.float32).reshape(block_pages, KVH, group_size, HD)
        scores = jnp.einsum('pkgd,pktd->pkgt', picked, key_block.astype(jnp.float32), precision=lax.Precision.HIGHEST) * score_scale
        live_mask = jnp.arange(PAGE, dtype=jnp.int32)[None, :] < fill_block[:, None]
        weight = jnp.where(live_mask[:, None, None, :], jnp.exp(scores - score_shift), 0.0)
        page_total = lax.optimization_barrier(jnp.sum(weight, axis=-1))
        rounded = lax.optimization_barrier(weight.astype(jnp.bfloat16)).astype(jnp.float32)
        page_sum = jnp.einsum('pkgt,pktd->pkgd', rounded, value_block.astype(jnp.float32), precision=lax.Precision.HIGHEST)
        numerator = numerator + jax.ops.segment_sum(page_sum, seq_block, num_segments=SEQS)
        denominator = denominator + jax.ops.segment_sum(page_total, seq_block, num_segments=SEQS)
        return ((numerator, denominator), None)
    start = (jnp.zeros((SEQS, KVH, group_size, HD), jnp.float32), jnp.zeros((SEQS, KVH, group_size), jnp.float32))
    (numerator, denominator), _ = lax.scan(visit, start, (key_blocks, value_blocks, seq_blocks, fill_blocks))
    result = numerator / denominator[..., None]
    return result.reshape(SEQS, HQ, HD).astype(jnp.bfloat16)
```

```python
import functools
import math

import jax
import jax.numpy as jnp
from jax import lax
from jax.experimental import pallas as pl
from jax.experimental.pallas import tpu as pltpu
from jax.sharding import PartitionSpec as P

HQ = 64
KVH = 8
GROUP = 16

score_shift = 8.0
log2_e = math.log2(math.e)


def direct(n):
    return n <= 8


def block_slot(block, rank, n):
    if not direct(n):
        return block
    if n & (n - 1) == 0:
        return block ^ rank
    return lax.rem(block - rank + n, n)


def fetch_pairs(n, s):
    if n & (n - 1) == 0:
        return [(i ^ s, i) for i in range(n)]
    return [((i + s) % n, i) for i in range(n)]


def table_kernel(
    lens, owner, local, keys, values, pos_out, page_out, fill_out, count_out, keys_out, values_out,
    sems, *, n, page_len
):
    loads = [
        pltpu.make_async_copy(keys, keys_out, sems.at[0]),
        pltpu.make_async_copy(values, values_out, sems.at[1]),
    ]
    for load in loads:
        load.start()
    rank = lax.axis_index("seq")
    seqs = owner.shape[0]
    own = seqs // n

    def visit_seq(b, count):
        length = lens[b]
        slots = lax.shift_right_logical(length + (page_len - 1), page_len.bit_length() - 1)
        block = b // own
        pos = block_slot(block, rank, n) * own + (b - block * own)

        def visit_slot(s, count):
            pos_out[count] = pos
            page_out[count] = local[b, s]
            fill_out[count] = jnp.minimum(length - s * page_len, page_len)
            return count + (owner[b, s] == rank).astype(jnp.int32)

        return lax.fori_loop(0, slots, visit_slot, count)

    count = lax.fori_loop(0, seqs, visit_seq, jnp.int32(0))
    for u in range(GROUP):
        pos_out[count + u] = 0
        page_out[count + u] = 0
        fill_out[count + u] = 0
    count_out[0] = lax.div(count + (GROUP - 1), GROUP)
    for load in loads:
        load.wait()


def attend_kernel(pos_t, page_t, fill_t, count, *refs, n, parts, kv):
    queries = refs[:parts]
    keys, values = refs[parts], refs[parts + 1]
    outs = refs[parts + 2 : parts + 2 + n]
    query, acc, wsum = refs[parts + 2 + n :]
    own = acc.shape[0] // n
    heads, head_dim = acc.shape[1], acc.shape[2]
    page_len = keys.shape[2]
    step = acc.shape[0] // parts
    for s in range(parts):
        query[pl.ds(s * step, step)] = queries[s][...]
    acc[...] = jnp.zeros_like(acc)
    wsum[...] = jnp.zeros_like(wsum)
    width = kv * page_len
    scale = log2_e / math.sqrt(head_dim)
    lane = lax.broadcasted_iota(jnp.int32, (heads, width), 1)
    row = lax.broadcasted_iota(jnp.int32, (heads, width), 0)
    token = jnp.where(
        lane // page_len == row // (heads // kv), lane % page_len, jnp.int32(page_len)
    )

    def visit(g, _):
        base = g * GROUP
        where = [pos_t[base + u] for u in range(GROUP)]
        pages = [page_t[base + u] for u in range(GROUP)]
        scores = [
            lax.dot_general(
                query[where[u]],
                keys[pages[u]].reshape(width, head_dim),
                (((1,), (1,)), ((), ())),
                preferred_element_type=jnp.float32,
            )
            for u in range(GROUP)
        ]
        weights = [
            jnp.where(
                token < fill_t[base + u],
                jnp.exp2(scores[u] * scale - score_shift * log2_e),
                0.0,
            )
            for u in range(GROUP)
        ]
        sums = [
            jnp.dot(
                weights[u].astype(jnp.bfloat16),
                values[pages[u]].reshape(width, head_dim),
                preferred_element_type=jnp.float32,
            )
            for u in range(GROUP)
        ]
        for u in range(GROUP):
            acc[where[u]] += sums[u]
            wsum[where[u]] += weights[u]
        return 0

    lax.fori_loop(0, count[0], visit, 0)
    lanes = lax.broadcasted_iota(jnp.int32, (heads, head_dim), 1)
    half = head_dim // 2
    for s in range(n):
        total = jnp.zeros((heads, head_dim), jnp.float32)
        for i in range(own):
            column = jnp.sum(wsum[s * own + i], axis=-1, keepdims=True)
            high = column.astype(jnp.bfloat16).astype(jnp.float32)
            total = jnp.where(lanes == i, high, total)
            total = jnp.where(lanes == half + i, column - high, total)
        outs[s][pl.ds(0, own)] = acc[pl.ds(s * own, own)].astype(outs[s].dtype)
        outs[s][own] = total.astype(outs[s].dtype)


def merge_kernel(*refs, own):
    out = refs[-1]
    total = refs[0][own].astype(jnp.float32)
    for ref in refs[1:-1]:
        total += ref[own].astype(jnp.float32)
    half = total.shape[1] // 2
    total = 1.0 / (total[:, :half] + total[:, half:])
    for i in range(own):
        numerator = refs[0][i].astype(jnp.float32)
        for ref in refs[1:-1]:
            numerator += ref[i].astype(jnp.float32)
        out[i] = (numerator * total[:, i : i + 1]).astype(out.dtype)


def body(queries, key_pages, value_pages, page_owner, page_local, seq_lengths):
    seq_count = page_owner.shape[0]
    pool_pages, kv_local, page_len, head_dim = key_pages.shape
    heads = kv_local * (HQ // KVH)
    n = lax.axis_size("seq")
    own = seq_count // n
    tp_rank = lax.axis_index("tp")
    mine = lax.dynamic_slice_in_dim(queries, tp_rank * heads, heads, 1)
    if direct(n):
        parts = [mine] + [lax.ppermute(mine, "seq", fetch_pairs(n, s)) for s in range(1, n)]
    else:
        parts = [lax.all_gather(mine, "seq", axis=0, tiled=True)]
    smem = pl.BlockSpec(memory_space=pltpu.SMEM)
    vmem = pl.BlockSpec(memory_space=pltpu.VMEM)
    table = jax.ShapeDtypeStruct((pool_pages + GROUP + 1,), jnp.int32)
    hbm = pl.BlockSpec(memory_space=pltpu.HBM)
    *tables, keys, values = pl.pallas_call(
        functools.partial(table_kernel, n=n, page_len=page_len),
        out_shape=[
            table,
            table,
            table,
            jax.ShapeDtypeStruct((1,), jnp.int32),
            jax.ShapeDtypeStruct(key_pages.shape, key_pages.dtype),
            jax.ShapeDtypeStruct(value_pages.shape, value_pages.dtype),
        ],
        in_specs=[smem] * 3 + [hbm] * 2,
        out_specs=[smem] * 4 + [vmem] * 2,
        scratch_shapes=[pltpu.SemaphoreType.DMA((2,))],
        compiler_params=pltpu.CompilerParams(vmem_limit_bytes=1024 * 1024),
        name="tables",
    )(seq_lengths, page_owner, page_local, key_pages, value_pages)
    sent = jax.ShapeDtypeStruct((own + 1, heads, head_dim), jnp.bfloat16)
    kept = jax.ShapeDtypeStruct((own + 1, heads, head_dim), jnp.float32)
    if direct(n):
        shapes = [kept] + [sent] * (n - 1)
    else:
        shapes = [sent] * n
    partial = pl.pallas_call(
        functools.partial(attend_kernel, n=n, parts=len(parts), kv=kv_local),
        out_shape=shapes,
        in_specs=[smem] * 4 + [vmem] * (len(parts) + 2),
        out_specs=[vmem] * n,
        scratch_shapes=[
            pltpu.VMEM((seq_count, heads, head_dim), jnp.bfloat16),
            pltpu.VMEM((seq_count, heads, head_dim), jnp.float32),
            pltpu.VMEM((seq_count, heads, kv_local * page_len), jnp.float32),
        ],
        compiler_params=pltpu.CompilerParams(vmem_limit_bytes=8 * 1024 * 1024),
        name="attend",
    )(*tables, *parts, keys, values)
    if direct(n):
        pieces = [partial[0]]
        for s in range(1, n):
            pairs = [(b, a) for a, b in fetch_pairs(n, s)]
            pieces.append(lax.ppermute(partial[s], "seq", pairs))
    else:
        arrived = lax.all_to_all(jnp.stack(partial), "seq", 0, 0)
        pieces = [arrived[s] for s in range(n)]
    return pl.pallas_call(
        functools.partial(merge_kernel, own=own),
        out_shape=jax.ShapeDtypeStruct((own, heads, head_dim), jnp.bfloat16),
        in_specs=[vmem] * n,
        out_specs=vmem,
        compiler_params=pltpu.CompilerParams(vmem_limit_bytes=4 * 1024 * 1024),
        name="merge",
    )(*pieces)


def solution(mesh):
    placed = (
        P(("rep", "seq"), None, None),
        P(("rep", "seq"), "tp", None, None),
        P(("rep", "seq"), "tp", None, None),
        P("rep", None),
        P("rep", None),
        P("rep"),
    )
    return jax.shard_map(
        body, mesh=mesh, in_specs=placed, out_specs=P(("rep", "seq"), "tp", None), check_vma=False
    )
```

```python
import functools
import math

import jax
import jax.numpy as jnp
from jax import lax
from jax.experimental import pallas as pl
from jax.experimental.pallas import tpu as pltpu
from jax.sharding import PartitionSpec as P

HQ = 64
KVH = 8
GROUP = 16
LOADS = 4

score_shift = 8.0
log2_e = math.log2(math.e)


def direct(n):
    return n <= 8


def block_slot(block, rank, n):
    if not direct(n):
        return block
    if n & (n - 1) == 0:
        return block ^ rank
    return lax.rem(block - rank + n, n)


def fetch_pairs(n, s):
    if n & (n - 1) == 0:
        return [(i ^ s, i) for i in range(n)]
    return [((i + s) % n, i) for i in range(n)]


def table_kernel(
    lens_in, owner_in, local_in, keys, values, pos_out, page_out, fill_out, count_out, keys_out,
    values_out, lens, owner, local, sems, *, n, page_len
):
    small = [
        pltpu.make_async_copy(lens_in, lens, sems.at[0]),
        pltpu.make_async_copy(owner_in, owner, sems.at[1]),
        pltpu.make_async_copy(local_in, local, sems.at[2]),
    ]
    cut = keys.shape[0] // LOADS
    loads = []
    for j in range(LOADS):
        part = pl.ds(j * cut, cut)
        loads.append(pltpu.make_async_copy(keys.at[part], keys_out.at[part], sems.at[3 + 2 * j]))
        loads.append(pltpu.make_async_copy(values.at[part], values_out.at[part], sems.at[4 + 2 * j]))
    for load in small + loads:
        load.start()
    for load in small:
        load.wait()
    rank = lax.axis_index("seq")
    seqs = owner.shape[0]
    own = seqs // n

    def visit_seq(b, count):
        length = lens[b]
        slots = lax.shift_right_logical(length + (page_len - 1), page_len.bit_length() - 1)
        block = b // own
        pos = block_slot(block, rank, n) * own + (b - block * own)

        def visit_slot(s, count):
            pos_out[count] = pos
            page_out[count] = local[b, s]
            fill_out[count] = jnp.minimum(length - s * page_len, page_len)
            return count + (owner[b, s] == rank).astype(jnp.int32)

        return lax.fori_loop(0, slots, visit_slot, count)

    count = lax.fori_loop(0, seqs, visit_seq, jnp.int32(0))
    for u in range(GROUP):
        pos_out[count + u] = 0
        page_out[count + u] = 0
        fill_out[count + u] = 0
    count_out[0] = lax.div(count + (GROUP - 1), GROUP)
    for load in loads:
        load.wait()


def attend_kernel(pos_t, page_t, fill_t, count, *refs, n, parts, kv):
    queries = refs[:parts]
    keys, values = refs[parts], refs[parts + 1]
    outs = refs[parts + 2 : parts + 2 + n]
    query, acc, wsum = refs[parts + 2 + n :]
    own = acc.shape[0] // n
    heads, head_dim = acc.shape[1], acc.shape[2]
    page_len = keys.shape[2]
    step = acc.shape[0] // parts
    for s in range(parts):
        query[pl.ds(s * step, step)] = queries[s][...]
    acc[...] = jnp.zeros_like(acc)
    wsum[...] = jnp.zeros_like(wsum)
    width = kv * page_len
    scale = log2_e / math.sqrt(head_dim)
    lane = lax.broadcasted_iota(jnp.int32, (heads, width), 1)
    row = lax.broadcasted_iota(jnp.int32, (heads, width), 0)
    token = jnp.where(
        lane // page_len == row // (heads // kv), lane % page_len, jnp.int32(page_len)
    )

    def visit(g, _):
        base = g * GROUP
        where = [pos_t[base + u] for u in range(GROUP)]
        pages = [page_t[base + u] for u in range(GROUP)]
        scores = [
            lax.dot_general(
                query[where[u]],
                keys[pages[u]].reshape(width, head_dim),
                (((1,), (1,)), ((), ())),
                preferred_element_type=jnp.float32,
            )
            for u in range(GROUP)
        ]
        weights = [
            jnp.where(
                token < fill_t[base + u],
                jnp.exp2(scores[u] * scale - score_shift * log2_e),
                0.0,
            )
            for u in range(GROUP)
        ]
        sums = [
            jnp.dot(
                weights[u].astype(jnp.bfloat16),
                values[pages[u]].reshape(width, head_dim),
                preferred_element_type=jnp.float32,
            )
            for u in range(GROUP)
        ]
        for u in range(GROUP):
            acc[where[u]] += sums[u]
            wsum[where[u]] += weights[u]
        return 0

    lax.fori_loop(0, count[0], visit, 0)
    lanes = lax.broadcasted_iota(jnp.int32, (heads, head_dim), 1)
    half = head_dim // 2
    for s in range(n):
        total = jnp.zeros((heads, head_dim), jnp.float32)
        for i in range(own):
            column = jnp.sum(wsum[s * own + i], axis=-1, keepdims=True)
            high = column.astype(jnp.bfloat16).astype(jnp.float32)
            total = jnp.where(lanes == i, high, total)
            total = jnp.where(lanes == half + i, column - high, total)
        outs[s][pl.ds(0, own)] = acc[pl.ds(s * own, own)].astype(outs[s].dtype)
        outs[s][own] = total.astype(outs[s].dtype)


def merge_kernel(*refs, own):
    out = refs[-1]
    total = refs[0][own].astype(jnp.float32)
    for ref in refs[1:-1]:
        total += ref[own].astype(jnp.float32)
    half = total.shape[1] // 2
    total = 1.0 / (total[:, :half] + total[:, half:])
    for i in range(own):
        numerator = refs[0][i].astype(jnp.float32)
        for ref in refs[1:-1]:
            numerator += ref[i].astype(jnp.float32)
        out[i] = (numerator * total[:, i : i + 1]).astype(out.dtype)


def body(queries, key_pages, value_pages, page_owner, page_local, seq_lengths):
    seq_count = page_owner.shape[0]
    pool_pages, kv_local, page_len, head_dim = key_pages.shape
    heads = kv_local * (HQ // KVH)
    n = lax.axis_size("seq")
    own = seq_count // n
    tp_rank = lax.axis_index("tp")
    mine = lax.dynamic_slice_in_dim(queries, tp_rank * heads, heads, 1)
    if direct(n):
        parts = [mine] + [lax.ppermute(mine, "seq", fetch_pairs(n, s)) for s in range(1, n)]
    else:
        parts = [lax.all_gather(mine, "seq", axis=0, tiled=True)]
    smem = pl.BlockSpec(memory_space=pltpu.SMEM)
    vmem = pl.BlockSpec(memory_space=pltpu.VMEM)
    table = jax.ShapeDtypeStruct((pool_pages + GROUP + 1,), jnp.int32)
    hbm = pl.BlockSpec(memory_space=pltpu.HBM)
    held = (seq_lengths, page_owner, page_local, key_pages, value_pages)
    *tables, keys, values = pl.pallas_call(
        functools.partial(table_kernel, n=n, page_len=page_len),
        out_shape=[
            table,
            table,
            table,
            jax.ShapeDtypeStruct((1,), jnp.int32),
            jax.ShapeDtypeStruct(key_pages.shape, key_pages.dtype),
            jax.ShapeDtypeStruct(value_pages.shape, value_pages.dtype),
        ],
        in_specs=[hbm] * 5,
        out_specs=[smem] * 4 + [vmem] * 2,
        scratch_shapes=[
            pltpu.SMEM(seq_lengths.shape, jnp.int32),
            pltpu.SMEM(page_owner.shape, jnp.int32),
            pltpu.SMEM(page_local.shape, jnp.int32),
            pltpu.SemaphoreType.DMA((3 + 2 * LOADS,)),
        ],
        compiler_params=pltpu.CompilerParams(vmem_limit_bytes=1024 * 1024),
        name="tables",
    )(*[pltpu.with_memory_space_constraint(x, pltpu.HBM) for x in held])
    sent = jax.ShapeDtypeStruct((own + 1, heads, head_dim), jnp.bfloat16)
    kept = jax.ShapeDtypeStruct((own + 1, heads, head_dim), jnp.float32)
    if direct(n):
        shapes = [kept] + [sent] * (n - 1)
    else:
        shapes = [sent] * n
    partial = pl.pallas_call(
        functools.partial(attend_kernel, n=n, parts=len(parts), kv=kv_local),
        out_shape=shapes,
        in_specs=[smem] * 4 + [vmem] * (len(parts) + 2),
        out_specs=[vmem] * n,
        scratch_shapes=[
            pltpu.VMEM((seq_count, heads, head_dim), jnp.bfloat16),
            pltpu.VMEM((seq_count, heads, head_dim), jnp.float32),
            pltpu.VMEM((seq_count, heads, kv_local * page_len), jnp.float32),
        ],
        compiler_params=pltpu.CompilerParams(vmem_limit_bytes=8 * 1024 * 1024),
        name="attend",
    )(*tables, *parts, keys, values)
    if direct(n):
        pieces = [partial[0]]
        for s in range(1, n):
            pairs = [(b, a) for a, b in fetch_pairs(n, s)]
            pieces.append(lax.ppermute(partial[s], "seq", pairs))
    else:
        arrived = lax.all_to_all(jnp.stack(partial), "seq", 0, 0)
        pieces = [arrived[s] for s in range(n)]
    return pl.pallas_call(
        functools.partial(merge_kernel, own=own),
        out_shape=jax.ShapeDtypeStruct((own, heads, head_dim), jnp.bfloat16),
        in_specs=[vmem] * n,
        out_specs=vmem,
        compiler_params=pltpu.CompilerParams(vmem_limit_bytes=4 * 1024 * 1024),
        name="merge",
    )(*pieces)


def solution(mesh):
    placed = (
        P(("rep", "seq"), None, None),
        P(("rep", "seq"), "tp", None, None),
        P(("rep", "seq"), "tp", None, None),
        P("rep", None),
        P("rep", None),
        P("rep"),
    )
    return jax.shard_map(
        body, mesh=mesh, in_specs=placed, out_specs=P(("rep", "seq"), "tp", None), check_vma=False
    )
```

```python
import functools
import math

import jax
import jax.numpy as jnp
from jax import lax
from jax.experimental import pallas as pl
from jax.experimental.pallas import tpu as pltpu
from jax.sharding import PartitionSpec as P

HQ = 64
KVH = 8
GROUP = 16
LOADS = 4

score_shift = 8.0
log2_e = math.log2(math.e)


def direct(n):
    return n <= 8


def halves(n):
    return [(n // 2, n), (0, n // 2)] if direct(n) and n > 1 else [(0, n)]


def block_of(slot, rank, n):
    if not direct(n):
        return slot
    if n & (n - 1) == 0:
        return slot ^ rank
    return lax.rem(slot + rank, n)


def fetch_pairs(n, s):
    if n & (n - 1) == 0:
        return [(i ^ s, i) for i in range(n)]
    return [((i + s) % n, i) for i in range(n)]


def table_kernel(
    lens_in, owner_in, local_in, keys, values, pos_out, page_out, fill_out, count_out, keys_out,
    values_out, lens, owner, local, sems, *, n, page_len
):
    small = [
        pltpu.make_async_copy(lens_in, lens, sems.at[0]),
        pltpu.make_async_copy(owner_in, owner, sems.at[1]),
        pltpu.make_async_copy(local_in, local, sems.at[2]),
    ]
    cut = keys.shape[0] // LOADS
    loads = []
    for j in range(LOADS):
        part = pl.ds(j * cut, cut)
        loads.append(pltpu.make_async_copy(keys.at[part], keys_out.at[part], sems.at[3 + 2 * j]))
        loads.append(pltpu.make_async_copy(values.at[part], values_out.at[part], sems.at[4 + 2 * j]))
    for load in small + loads:
        load.start()
    for load in small:
        load.wait()
    rank = lax.axis_index("seq")
    seqs = owner.shape[0]
    own = seqs // n

    def visit_seq(p, count, first):
        slot = p // own
        b = block_of(slot, rank, n) * own + (p - slot * own)
        length = lens[b]
        slots = lax.shift_right_logical(length + (page_len - 1), page_len.bit_length() - 1)
        pos = p - first

        def visit_slot(s, count):
            pos_out[count] = pos
            page_out[count] = local[b, s]
            fill_out[count] = jnp.minimum(length - s * page_len, page_len)
            return count + (owner[b, s] == rank).astype(jnp.int32)

        return lax.fori_loop(0, slots, visit_slot, count)

    count = jnp.int32(0)
    count_out[0] = count
    for h, (low, high) in enumerate(halves(n)):
        count = lax.fori_loop(
            low * own, high * own, functools.partial(visit_seq, first=low * own), count
        )
        for u in range(GROUP):
            pos_out[count + u] = 0
            page_out[count + u] = 0
            fill_out[count + u] = 0
        groups = lax.div(count + (GROUP - 1), GROUP)
        count_out[h + 1] = groups
        count = groups * GROUP
    for load in loads:
        load.wait()


def attend_kernel(pos_t, page_t, fill_t, count, *refs, n, parts, kv, half_at):
    queries = refs[:parts]
    keys, values = refs[parts], refs[parts + 1]
    outs = refs[parts + 2 : parts + 2 + n]
    query, acc, wsum = refs[parts + 2 + n :]
    own = acc.shape[0] // n
    heads, head_dim = acc.shape[1], acc.shape[2]
    page_len = keys.shape[2]
    step = acc.shape[0] // parts
    for s in range(parts):
        query[pl.ds(s * step, step)] = queries[s][...]
    acc[...] = jnp.zeros_like(acc)
    wsum[...] = jnp.zeros_like(wsum)
    width = kv * page_len
    scale = log2_e / math.sqrt(head_dim)
    lane = lax.broadcasted_iota(jnp.int32, (heads, width), 1)
    row = lax.broadcasted_iota(jnp.int32, (heads, width), 0)
    token = jnp.where(
        lane // page_len == row // (heads // kv), lane % page_len, jnp.int32(page_len)
    )

    def visit(g, _):
        base = g * GROUP
        where = [pos_t[base + u] for u in range(GROUP)]
        pages = [page_t[base + u] for u in range(GROUP)]
        scores = [
            lax.dot_general(
                query[where[u]],
                keys[pages[u]].reshape(width, head_dim),
                (((1,), (1,)), ((), ())),
                preferred_element_type=jnp.float32,
            )
            for u in range(GROUP)
        ]
        weights = [
            jnp.where(
                token < fill_t[base + u],
                jnp.exp2(scores[u] * scale - score_shift * log2_e),
                0.0,
            )
            for u in range(GROUP)
        ]
        sums = [
            jnp.dot(
                weights[u].astype(jnp.bfloat16),
                values[pages[u]].reshape(width, head_dim),
                preferred_element_type=jnp.float32,
            )
            for u in range(GROUP)
        ]
        for u in range(GROUP):
            acc[where[u]] += sums[u]
            wsum[where[u]] += weights[u]
        return 0

    lax.fori_loop(count[half_at], count[half_at + 1], visit, 0)
    lanes = lax.broadcasted_iota(jnp.int32, (heads, head_dim), 1)
    half = head_dim // 2
    for s in range(n):
        total = jnp.zeros((heads, head_dim), jnp.float32)
        for i in range(own):
            column = jnp.sum(wsum[s * own + i], axis=-1, keepdims=True)
            high = column.astype(jnp.bfloat16).astype(jnp.float32)
            total = jnp.where(lanes == i, high, total)
            total = jnp.where(lanes == half + i, column - high, total)
        outs[s][pl.ds(0, own)] = acc[pl.ds(s * own, own)].astype(outs[s].dtype)
        outs[s][own] = total.astype(outs[s].dtype)


def merge_kernel(*refs, own):
    out = refs[-1]
    total = refs[0][own].astype(jnp.float32)
    for ref in refs[1:-1]:
        total += ref[own].astype(jnp.float32)
    half = total.shape[1] // 2
    total = 1.0 / (total[:, :half] + total[:, half:])
    for i in range(own):
        numerator = refs[0][i].astype(jnp.float32)
        for ref in refs[1:-1]:
            numerator += ref[i].astype(jnp.float32)
        out[i] = (numerator * total[:, i : i + 1]).astype(out.dtype)


def body(queries, key_pages, value_pages, page_owner, page_local, seq_lengths):
    seq_count = page_owner.shape[0]
    pool_pages, kv_local, page_len, head_dim = key_pages.shape
    heads = kv_local * (HQ // KVH)
    n = lax.axis_size("seq")
    own = seq_count // n
    tp_rank = lax.axis_index("tp")
    mine = lax.dynamic_slice_in_dim(queries, tp_rank * heads, heads, 1)
    if direct(n):
        parts = [mine] + [lax.ppermute(mine, "seq", fetch_pairs(n, s)) for s in range(1, n)]
    else:
        parts = [lax.all_gather(mine, "seq", axis=0, tiled=True)]
    smem = pl.BlockSpec(memory_space=pltpu.SMEM)
    vmem = pl.BlockSpec(memory_space=pltpu.VMEM)
    table = jax.ShapeDtypeStruct((pool_pages + 2 * GROUP + 1,), jnp.int32)
    hbm = pl.BlockSpec(memory_space=pltpu.HBM)
    held = (seq_lengths, page_owner, page_local, key_pages, value_pages)
    *tables, keys, values = pl.pallas_call(
        functools.partial(table_kernel, n=n, page_len=page_len),
        out_shape=[
            table,
            table,
            table,
            jax.ShapeDtypeStruct((len(halves(n)) + 1,), jnp.int32),
            jax.ShapeDtypeStruct(key_pages.shape, key_pages.dtype),
            jax.ShapeDtypeStruct(value_pages.shape, value_pages.dtype),
        ],
        in_specs=[hbm] * 5,
        out_specs=[smem] * 4 + [vmem] * 2,
        scratch_shapes=[
            pltpu.SMEM(seq_lengths.shape, jnp.int32),
            pltpu.SMEM(page_owner.shape, jnp.int32),
            pltpu.SMEM(page_local.shape, jnp.int32),
            pltpu.SemaphoreType.DMA((3 + 2 * LOADS,)),
        ],
        compiler_params=pltpu.CompilerParams(vmem_limit_bytes=1024 * 1024),
        name="tables",
    )(*[pltpu.with_memory_space_constraint(x, pltpu.HBM) for x in held])
    sent = jax.ShapeDtypeStruct((own + 1, heads, head_dim), jnp.bfloat16)
    kept = jax.ShapeDtypeStruct((own + 1, heads, head_dim), jnp.float32)
    if direct(n):
        shapes = [kept] + [sent] * (n - 1)
    else:
        shapes = [sent] * n
    partial = [None] * n
    for h, (low, high) in enumerate(halves(n)):
        used = parts[low:high] if direct(n) else parts
        rows = (high - low) * own
        partial[low:high] = pl.pallas_call(
            functools.partial(
                attend_kernel, n=high - low, parts=len(used), kv=kv_local, half_at=h
            ),
            out_shape=shapes[low:high],
            in_specs=[smem] * 4 + [vmem] * (len(used) + 2),
            out_specs=[vmem] * (high - low),
            scratch_shapes=[
                pltpu.VMEM((rows, heads, head_dim), jnp.bfloat16),
                pltpu.VMEM((rows, heads, head_dim), jnp.float32),
                pltpu.VMEM((rows, heads, kv_local * page_len), jnp.float32),
            ],
            compiler_params=pltpu.CompilerParams(vmem_limit_bytes=8 * 1024 * 1024),
            name="attend",
        )(*tables, *used, keys, values)
    if direct(n):
        pieces = [partial[0]]
        for s in range(1, n):
            pairs = [(b, a) for a, b in fetch_pairs(n, s)]
            pieces.append(lax.ppermute(partial[s], "seq", pairs))
    else:
        arrived = lax.all_to_all(jnp.stack(partial), "seq", 0, 0)
        pieces = [arrived[s] for s in range(n)]
    return pl.pallas_call(
        functools.partial(merge_kernel, own=own),
        out_shape=jax.ShapeDtypeStruct((own, heads, head_dim), jnp.bfloat16),
        in_specs=[vmem] * n,
        out_specs=vmem,
        compiler_params=pltpu.CompilerParams(vmem_limit_bytes=4 * 1024 * 1024),
        name="merge",
    )(*pieces)


def solution(mesh):
    placed = (
        P(("rep", "seq"), None, None),
        P(("rep", "seq"), "tp", None, None),
        P(("rep", "seq"), "tp", None, None),
        P("rep", None),
        P("rep", None),
        P("rep"),
    )
    return jax.shard_map(
        body, mesh=mesh, in_specs=placed, out_specs=P(("rep", "seq"), "tp", None), check_vma=False
    )
```

```python
import functools
import math

import jax
import jax.numpy as jnp
from jax import lax
from jax.experimental import pallas as pl
from jax.experimental.pallas import tpu as pltpu
from jax.sharding import PartitionSpec as P

HQ = 64
KVH = 8
GROUP = 16
LOADS = 4

score_shift = 8.0
log2_e = math.log2(math.e)


def direct(n):
    return n <= 8


def halves(n):
    return [(n // 2, n), (0, n // 2)] if direct(n) and n > 1 else [(0, n)]


def block_of(slot, rank, n):
    if not direct(n):
        return slot
    if n & (n - 1) == 0:
        return slot ^ rank
    return lax.rem(slot + rank, n)


def fetch_pairs(n, s):
    if n & (n - 1) == 0:
        return [(i ^ s, i) for i in range(n)]
    return [((i + s) % n, i) for i in range(n)]


def table_kernel(
    lens_in, owner_in, local_in, keys, values, pos_out, page_out, fill_out, count_out, keys_out,
    values_out, lens, owner, local, sems, *, n, page_len
):
    small = [
        pltpu.make_async_copy(lens_in, lens, sems.at[0]),
        pltpu.make_async_copy(owner_in, owner, sems.at[1]),
        pltpu.make_async_copy(local_in, local, sems.at[2]),
    ]
    cut = keys.shape[0] // LOADS
    loads = []
    for j in range(LOADS):
        part = pl.ds(j * cut, cut)
        loads.append(pltpu.make_async_copy(keys.at[part], keys_out.at[part], sems.at[3 + 2 * j]))
        loads.append(pltpu.make_async_copy(values.at[part], values_out.at[part], sems.at[4 + 2 * j]))
    for load in small + loads:
        load.start()
    for load in small:
        load.wait()
    rank = lax.axis_index("seq")
    seqs = owner.shape[0]
    own = seqs // n

    def visit_seq(i, count, start, first):
        b = start + i
        length = lens[b]
        slots = lax.shift_right_logical(length + (page_len - 1), page_len.bit_length() - 1)
        pos = first + i

        def visit_slot(s, count):
            pos_out[count] = pos
            page_out[count] = local[b, s]
            fill_out[count] = jnp.minimum(length - s * page_len, page_len)
            return count + (owner[b, s] == rank).astype(jnp.int32)

        return lax.fori_loop(0, slots, visit_slot, count)

    count = jnp.int32(0)
    count_out[0] = count
    for h, (low, high) in enumerate(halves(n)):
        for slot in range(low, high):
            start = block_of(slot, rank, n) * own
            visit = functools.partial(visit_seq, start=start, first=(slot - low) * own)
            count = lax.fori_loop(0, own, visit, count)
        for u in range(GROUP):
            pos_out[count + u] = 0
            page_out[count + u] = 0
            fill_out[count + u] = 0
        groups = lax.div(count + (GROUP - 1), GROUP)
        count_out[h + 1] = groups
        count = groups * GROUP
    for load in loads:
        load.wait()


def attend_kernel(pos_t, page_t, fill_t, count, *refs, n, parts, kv, half_at):
    queries = refs[:parts]
    keys, values = refs[parts], refs[parts + 1]
    outs = refs[parts + 2 : parts + 2 + n]
    query, acc, wsum = refs[parts + 2 + n :]
    own = acc.shape[0] // n
    heads, head_dim = acc.shape[1], acc.shape[2]
    page_len = keys.shape[2]
    step = acc.shape[0] // parts
    for s in range(parts):
        query[pl.ds(s * step, step)] = queries[s][...]
    acc[...] = jnp.zeros_like(acc)
    wsum[...] = jnp.zeros_like(wsum)
    width = kv * page_len
    scale = log2_e / math.sqrt(head_dim)
    lane = lax.broadcasted_iota(jnp.int32, (heads, width), 1)
    row = lax.broadcasted_iota(jnp.int32, (heads, width), 0)
    token = jnp.where(
        lane // page_len == row // (heads // kv), lane % page_len, jnp.int32(page_len)
    )

    def visit(g, _):
        base = g * GROUP
        where = [pos_t[base + u] for u in range(GROUP)]
        pages = [page_t[base + u] for u in range(GROUP)]
        scores = [
            lax.dot_general(
                query[where[u]],
                keys[pages[u]].reshape(width, head_dim),
                (((1,), (1,)), ((), ())),
                preferred_element_type=jnp.float32,
            )
            for u in range(GROUP)
        ]
        weights = [
            jnp.where(
                token < fill_t[base + u],
                jnp.exp2(scores[u] * scale - score_shift * log2_e),
                0.0,
            )
            for u in range(GROUP)
        ]
        sums = [
            jnp.dot(
                weights[u].astype(jnp.bfloat16),
                values[pages[u]].reshape(width, head_dim),
                preferred_element_type=jnp.float32,
            )
            for u in range(GROUP)
        ]
        for u in range(GROUP):
            acc[where[u]] += sums[u]
            wsum[where[u]] += weights[u]
        return 0

    lax.fori_loop(count[half_at], count[half_at + 1], visit, 0)
    lanes = lax.broadcasted_iota(jnp.int32, (heads, head_dim), 1)
    half = head_dim // 2
    for s in range(n):
        total = jnp.zeros((heads, head_dim), jnp.float32)
        for i in range(own):
            column = jnp.sum(wsum[s * own + i], axis=-1, keepdims=True)
            high = column.astype(jnp.bfloat16).astype(jnp.float32)
            total = jnp.where(lanes == i, high, total)
            total = jnp.where(lanes == half + i, column - high, total)
        outs[s][pl.ds(0, own)] = acc[pl.ds(s * own, own)].astype(outs[s].dtype)
        outs[s][own] = total.astype(outs[s].dtype)


def merge_kernel(*refs, own):
    out = refs[-1]
    total = refs[0][own].astype(jnp.float32)
    for ref in refs[1:-1]:
        total += ref[own].astype(jnp.float32)
    half = total.shape[1] // 2
    total = 1.0 / (total[:, :half] + total[:, half:])
    for i in range(own):
        numerator = refs[0][i].astype(jnp.float32)
        for ref in refs[1:-1]:
            numerator += ref[i].astype(jnp.float32)
        out[i] = (numerator * total[:, i : i + 1]).astype(out.dtype)


def body(queries, key_pages, value_pages, page_owner, page_local, seq_lengths):
    seq_count = page_owner.shape[0]
    pool_pages, kv_local, page_len, head_dim = key_pages.shape
    heads = kv_local * (HQ // KVH)
    n = lax.axis_size("seq")
    own = seq_count // n
    tp_rank = lax.axis_index("tp")
    mine = lax.dynamic_slice_in_dim(queries, tp_rank * heads, heads, 1)
    if direct(n):
        parts = [mine] + [lax.ppermute(mine, "seq", fetch_pairs(n, s)) for s in range(1, n)]
    else:
        parts = [lax.all_gather(mine, "seq", axis=0, tiled=True)]
    smem = pl.BlockSpec(memory_space=pltpu.SMEM)
    vmem = pl.BlockSpec(memory_space=pltpu.VMEM)
    table = jax.ShapeDtypeStruct((pool_pages + 2 * GROUP + 1,), jnp.int32)
    hbm = pl.BlockSpec(memory_space=pltpu.HBM)
    held = (seq_lengths, page_owner, page_local, key_pages, value_pages)
    *tables, keys, values = pl.pallas_call(
        functools.partial(table_kernel, n=n, page_len=page_len),
        out_shape=[
            table,
            table,
            table,
            jax.ShapeDtypeStruct((len(halves(n)) + 1,), jnp.int32),
            jax.ShapeDtypeStruct(key_pages.shape, key_pages.dtype),
            jax.ShapeDtypeStruct(value_pages.shape, value_pages.dtype),
        ],
        in_specs=[hbm] * 5,
        out_specs=[smem] * 4 + [vmem] * 2,
        scratch_shapes=[
            pltpu.SMEM(seq_lengths.shape, jnp.int32),
            pltpu.SMEM(page_owner.shape, jnp.int32),
            pltpu.SMEM(page_local.shape, jnp.int32),
            pltpu.SemaphoreType.DMA((3 + 2 * LOADS,)),
        ],
        compiler_params=pltpu.CompilerParams(vmem_limit_bytes=1024 * 1024),
        name="tables",
    )(*[pltpu.with_memory_space_constraint(x, pltpu.HBM) for x in held])
    sent = jax.ShapeDtypeStruct((own + 1, heads, head_dim), jnp.bfloat16)
    kept = jax.ShapeDtypeStruct((own + 1, heads, head_dim), jnp.float32)
    if direct(n):
        shapes = [kept] + [sent] * (n - 1)
    else:
        shapes = [sent] * n
    partial = [None] * n
    for h, (low, high) in enumerate(halves(n)):
        used = parts[low:high] if direct(n) else parts
        rows = (high - low) * own
        partial[low:high] = pl.pallas_call(
            functools.partial(
                attend_kernel, n=high - low, parts=len(used), kv=kv_local, half_at=h
            ),
            out_shape=shapes[low:high],
            in_specs=[smem] * 4 + [vmem] * (len(used) + 2),
            out_specs=[vmem] * (high - low),
            scratch_shapes=[
                pltpu.VMEM((rows, heads, head_dim), jnp.bfloat16),
                pltpu.VMEM((rows, heads, head_dim), jnp.float32),
                pltpu.VMEM((rows, heads, kv_local * page_len), jnp.float32),
            ],
            compiler_params=pltpu.CompilerParams(vmem_limit_bytes=8 * 1024 * 1024),
            name="attend",
        )(*tables, *used, keys, values)
    if direct(n):
        pieces = [partial[0]]
        for s in range(1, n):
            pairs = [(b, a) for a, b in fetch_pairs(n, s)]
            pieces.append(lax.ppermute(partial[s], "seq", pairs))
    else:
        arrived = lax.all_to_all(jnp.stack(partial), "seq", 0, 0)
        pieces = [arrived[s] for s in range(n)]
    return pl.pallas_call(
        functools.partial(merge_kernel, own=own),
        out_shape=jax.ShapeDtypeStruct((own, heads, head_dim), jnp.bfloat16),
        in_specs=[vmem] * n,
        out_specs=vmem,
        compiler_params=pltpu.CompilerParams(vmem_limit_bytes=4 * 1024 * 1024),
        name="merge",
    )(*pieces)


def solution(mesh):
    placed = (
        P(("rep", "seq"), None, None),
        P(("rep", "seq"), "tp", None, None),
        P(("rep", "seq"), "tp", None, None),
        P("rep", None),
        P("rep", None),
        P("rep"),
    )
    return jax.shard_map(
        body, mesh=mesh, in_specs=placed, out_specs=P(("rep", "seq"), "tp", None), check_vma=False
    )
```
